32 devices in a mesh: dp: 8 (over y, x, core), vocab: 4 (over z).
Axes of the slice: x: 2, y: 2, z: 4, core: 2. Of those that a mesh axis runs over, the one named last changes fastest.
Arguments:
- resid: bfloat16 [2, 1024, 4096], P(None, 'dp'), may hold values from -6 to 6
- norm_gain: float32 [4096], replicated, may hold values from 0.5 to 1.5
- in_x: bfloat16 [4096, 4096], P('dp', 'vocab'), may hold values from -0.09375 to 0.09375
- in_z: bfloat16 [4096, 4096], P('dp', 'vocab'), may hold values from -0.09375 to 0.09375
- conv_w: float32 [4, 4096], P(None, 'vocab'), may hold values from -3 to 3
- conv_b: float32 [4096], P('vocab'), may hold values from -3 to 3
- xdt_w: bfloat16 [4096, 256], P('vocab'), may hold values from -0.09375 to 0.09375
- xbc_w: bfloat16 [4096, 32], P('vocab'), may hold values from -0.09375 to 0.09375
- dt_gain: float32 [256], replicated, may hold values from 0.5 to 1.5
- dt_proj: bfloat16 [256, 4096], P(None, 'vocab'), may hold values from -0.375 to 0.375
- dt_bias: float32 [4096], P('vocab'), may hold values from -4 to 1
- a_rate: float32 [4096, 16], P('vocab'), may hold values from 0.0001 to 1
- out_w: bfloat16 [4096, 4096], P('vocab'), may hold values from -0.09375 to 0.09375
- final_gain: float32 [4096], replicated, may hold values from 0.5 to 1.5
- head_w: bfloat16 [8192, 4096], P('vocab', 'dp'), as said below
- targets: int32 [2, 1024], P(None, 'dp'), may hold values from 0 to 8191
- lengths: int32 [2], replicated, may hold values from 256 to 1024
Outputs:
- hidden_out: bfloat16 [2, 1024, 4096], P(None, 'dp', 'vocab')
- token_logp: float32 [2, 1024], P(None, 'dp')
- mean_logp: float32 [], replicated
The draws below stay inside these ranges and needn't reach their ends.
Inputs may be any that keep to these rules, and one draw needn't show every extreme that they name: `head_w`: entries lie within 720 / sqrt(4096) of zero.
All inputs are finite; a program needn't handle non-finite values.
Results may differ from the reference program's by a relative error of at most 0.019.
Values may be sent and summed in bfloat16 or wider, within the bound.
A program may use at most 128 MiB of HBM per device.

```python
import math
import jax
import jax.numpy as jnp
from jax import lax

D = 4096
N = 16
R = 256
KCONV = 4
B = 2
L = 1024
E = 4096
V = 8192


def draw_head_w(key, part):
    values = jnp.clip(jax.random.normal(key, (V, D), jnp.float32), -6.0, 6.0) * (3.0 / math.sqrt(D))
    return values.astype(jnp.bfloat16)


def plant(entries, key, least, largest):
    spot = [jax.random.randint(jax.random.fold_in(key, axis), (), 0, length) for axis, length in enumerate(entries.shape)]
    main_axis = entries.shape.index(max(entries.shape))
    beside = spot[:main_axis] + [(spot[main_axis] + 1) % entries.shape[main_axis]] + spot[main_axis + 1:]
    return entries.at[tuple(spot)].set(least).at[tuple(beside)].set(largest)


def steps_of(key, extent, shards, low, largest):
    loudness, own = 1.0, jax.random.fold_in(key, 6)
    for position, shards_of in shards:
        steps = jnp.exp(jax.random.uniform(jax.random.fold_in(own, position), (shards_of,), jnp.float32, low / len(shards), largest / len(shards)))
        loudness = loudness * jnp.repeat(steps, extent[position] // shards_of).reshape([-1 if axis == position else 1 for axis in range(len(extent))])
    return loudness


def normal_values(key, extent, width, most, split=(), kind=jnp.bfloat16):
    array = jax.random.normal(key, extent, jnp.float32) * width
    if len(split) > 0:
        array = steps_of(key, extent, split, -0.22, 0.18) * array
    return jnp.clip(array, min=-most, max=most).astype(kind)


def setup_inputs(seed: int = 0) -> dict:
    keys = jax.random.split(jax.random.key(seed), 18)
    return {
        "resid": normal_values(keys[0], (B, L, D), 1.0, 6.0, ((1, 8),)),
        "norm_gain": jnp.clip(1.0 + 0.1 * jax.random.normal(keys[1], (D,), jnp.float32), 0.5, 1.5),
        "in_x": normal_values(keys[2], (D, E), D ** -0.5, 0.09375, ((0, 8), (1, 4))),
        "in_z": normal_values(keys[3], (D, E), D ** -0.5, 0.09375, ((0, 8), (1, 4))),
        "conv_w": normal_values(keys[4], (KCONV, E), 0.5, 3.0, ((1, 4),), jnp.float32),
        "conv_b": normal_values(keys[5], (E,), 0.5, 3.0, ((0, 4),), jnp.float32),
        "xdt_w": normal_values(keys[6], (E, R), E ** -0.5, 0.09375, ((0, 4),)),
        "xbc_w": normal_values(keys[7], (E, 2 * N), E ** -0.5, 0.09375, ((0, 4),)),
        "dt_gain": jnp.clip(1.0 + 0.1 * jax.random.normal(keys[8], (R,), jnp.float32), 0.5, 1.5),
        "dt_proj": normal_values(keys[9], (R, E), R ** -0.5, 0.375, ((1, 4),)),
        "dt_bias": jnp.clip(-4.0 + 5.0 * jax.random.uniform(keys[10], (E,), jnp.float32) ** steps_of(keys[10], (E,), ((0, 4),), -0.2, 0.2), -4.0, 1.0),
        "a_rate": jnp.clip(jnp.exp(math.log(1.0) - 9.2103404 * jax.random.uniform(keys[11], (E, N), jnp.float32) ** steps_of(keys[11], (E, N), ((0, 4),), -0.2, 0.2)), 0.0001, 1.0),
        "out_w": normal_values(keys[12], (E, D), E ** -0.5, 0.09375, ((0, 4),)),
        "final_gain": jnp.clip(1.0 + 0.1 * jax.random.normal(keys[13], (D,), jnp.float32), 0.5, 1.5),
        "head_w": draw_head_w(jax.random.fold_in(keys[17], 71), 0),
        "targets": plant(jax.random.randint(keys[15], (B, L), 0, V), jax.random.fold_in(keys[15], 1), 0, V - 1).astype(jnp.int32),
        "lengths": jax.random.randint(keys[16], (B,), L // 4, L + 1).astype(jnp.int32),
    }


def rms_norm(values, gain, epsilon):
    return values * lax.rsqrt(lax.optimization_barrier(jnp.mean(values * values, axis=-1, keepdims=True)) + epsilon) * gain

def reference(resid, norm_gain, in_x, in_z, conv_w, conv_b, xdt_w, xbc_w, dt_gain, dt_proj, dt_bias, a_rate, out_w, final_gain, head_w, targets, lengths):
    stream = resid.astype(jnp.float32)
    normed = rms_norm(stream, norm_gain, 1e-05).astype(jnp.bfloat16).reshape(B * L, D)
    x_inner = jnp.dot(normed, in_x, preferred_element_type=jnp.float32).astype(jnp.bfloat16).reshape(B, L, E)
    z_gate = jnp.dot(normed, in_z, preferred_element_type=jnp.float32).astype(jnp.bfloat16).reshape(B, L, E)
    padded = jnp.pad(x_inner.astype(jnp.float32), ((0, 0), (KCONV - 1, 0), (0, 0)))
    conv_sum = jnp.zeros((B, L, E), jnp.float32) + conv_b
    for tap_index in range(KCONV):
        conv_sum = conv_sum + conv_w[tap_index] * padded[:, tap_index:tap_index + L, :]
    conv_act = jax.nn.silu(conv_sum)
    conv_low = conv_act.astype(jnp.bfloat16).reshape(B * L, E)
    dt_raw = jnp.dot(conv_low, xdt_w, preferred_element_type=jnp.float32)
    bc_raw = jnp.dot(conv_low, xbc_w, preferred_element_type=jnp.float32)
    dt_normed = rms_norm(dt_raw, dt_gain, 1e-06).astype(jnp.bfloat16)
    step_size = jax.nn.softplus(jnp.dot(dt_normed, dt_proj, preferred_element_type=jnp.float32) + dt_bias).reshape(B, L, E)
    in_map = bc_raw[:, :N].reshape(B, L, N)
    out_map = bc_raw[:, N:].reshape(B, L, N)

    def advance(carry_state, inputs):
        step_now, conv_now, in_now, out_now = inputs
        carry_state = jnp.exp(-step_now[..., None] * a_rate) * carry_state + (step_now * conv_now)[..., None] * in_now[:, None, :]
        return (carry_state, lax.optimization_barrier(jnp.sum(carry_state * out_now[:, None, :], axis=-1)))
    start_state = jnp.zeros((B, E, N), jnp.float32)
    inputs = (step_size.transpose(1, 0, 2), conv_act.transpose(1, 0, 2), in_map.transpose(1, 0, 2), out_map.transpose(1, 0, 2))
    _, scanned = lax.scan(advance, start_state, inputs)
    mixed = scanned.transpose(1, 0, 2)
    gated = (mixed * jax.nn.silu(z_gate.astype(jnp.float32))).astype(jnp.bfloat16).reshape(B * L, E)
    mixer_out = jnp.dot(gated, out_w, preferred_element_type=jnp.float32)
    hidden = (stream.reshape(B * L, D) + mixer_out).astype(jnp.bfloat16)
    final = rms_norm(hidden.astype(jnp.float32), final_gain, 1e-05).astype(jnp.bfloat16)
    logits = lax.dot_general(final, head_w, (((1,), (1,)), ((), ())), preferred_element_type=jnp.float32)
    row_top = lax.optimization_barrier(jnp.max(logits, axis=-1))
    log_total = row_top + jnp.log(lax.optimization_barrier(jnp.sum(jnp.exp(logits - row_top[:, None]), axis=-1)))
    picked = jnp.take_along_axis(logits, targets.reshape(B * L, 1).astype(jnp.int32), axis=1)[:, 0]
    token_logp = (picked - log_total).reshape(B, L)
    valid_mask = jnp.arange(L, dtype=jnp.int32)[None, :] < lengths[:, None]
    mean_logp = jnp.sum(jnp.where(valid_mask, token_logp, 0.0)) / jnp.sum(lengths.astype(jnp.float32))
    return (hidden.reshape(B, L, D), token_logp, mean_logp)
```

```python
import functools

import jax
import jax.numpy as jnp
from jax import lax
from jax.experimental import pallas as pl
from jax.experimental.pallas import tpu as pltpu
from jax.sharding import PartitionSpec as P

MESH = pl.DeviceIdType.MESH
VMEM = pl.BlockSpec(memory_space=pltpu.VMEM)
CHUNKS = 8
LANE = 128


def peer(axis, shift):
    size = lax.axis_size(axis)
    return {axis: lax.rem(lax.axis_index(axis) + shift, size)}


def greet(axes):
    barrier = pltpu.get_barrier_semaphore()
    count = 0
    for axis in axes:
        for shift in range(1, lax.axis_size(axis)):
            pl.semaphore_signal(barrier, inc=1, device_id=peer(axis, shift), device_id_type=MESH)
            count += 1
    pl.semaphore_wait(barrier, count)


def remote(src, dst, send_sem, recv_sem, device):
    return pltpu.make_async_remote_copy(
        src_ref=src, dst_ref=dst, send_sem=send_sem, recv_sem=recv_sem,
        device_id=device, device_id_type=MESH,
    )


def call(kernel, out_shape, scratch, cid, cost_us, name):
    return pl.pallas_call(
        kernel,
        out_shape=out_shape,
        scratch_shapes=scratch,
        compiler_params=pltpu.CompilerParams(
            collective_id=cid, has_side_effects=True, vmem_limit_bytes=56 * 1024 * 1024
        ),
        cost_estimate=pl.CostEstimate(
            flops=0, bytes_accessed=int(cost_us * 3.0e6), transcendentals=0
        ),
        name=name,
    )


def dt_kernel(nv, ranks, part_ref, gain_ref, out_ref, recv, mine, s1, r1, s2, r2):
    me = lax.axis_index("vocab")
    rows = part_ref.shape[0] // nv
    greet(("vocab",))
    copies = []
    for shift in range(1, nv):
        target = lax.rem(me + shift, nv)
        copy = remote(
            part_ref.at[pl.ds(pl.multiple_of(target * rows, rows), rows)], recv.at[shift - 1],
            s1.at[shift - 1], r1.at[shift - 1], peer("vocab", shift),
        )
        copy.start()
        copies.append(copy)
    own = pl.ds(pl.multiple_of(me * rows, rows), rows)
    total = part_ref[own, :].astype(jnp.float32)
    for shift in range(1, nv):
        copies[shift - 1].wait()
        total = total + recv[shift - 1].astype(jnp.float32)
    dt = total[:, :ranks]
    scale = lax.rsqrt(jnp.mean(dt * dt, axis=-1, keepdims=True) + 1e-06)
    mine[:, :ranks] = (dt * scale * gain_ref[...]).astype(jnp.bfloat16)
    mine[:, ranks:] = total[:, ranks:].astype(jnp.bfloat16)
    copies = []
    for shift in range(1, nv):
        copy = remote(
            mine, out_ref.at[own], s2.at[shift - 1], r2.at[shift - 1], peer("vocab", shift)
        )
        copy.start()
        copies.append(copy)
    out_ref[own, :] = mine[...]
    for copy in copies:
        copy.wait()


def dt_reduce(part, gain, nv, ranks):
    rows, cols = part.shape
    sems = [pltpu.SemaphoreType.DMA((nv - 1,))] * 4
    return call(
        functools.partial(dt_kernel, nv, ranks),
        jax.ShapeDtypeStruct((rows, cols), jnp.bfloat16),
        [
            pltpu.VMEM((nv - 1, rows // nv, cols), jnp.bfloat16),
            pltpu.VMEM((rows // nv, cols), jnp.bfloat16),
        ] + sems,
        1, 10, "dt_reduce",
    )(part, gain)


def scan_kernel(
    nd, batch, nstate, ranks, low_ref, proj_ref, bias_ref, conv_ref, rate_ref, out_ref,
    step, drive, maps, result, state, sums, agg, tot, agg_in, tot_in, s1, r1, s2, r2,
):
    me = lax.axis_index("dp")
    rows, chans = conv_ref.shape
    lanes = chans // LANE
    length = rows // batch
    span = length // CHUNKS
    greet(("dp",))
    low_dt = low_ref[:, :ranks]
    maps[...] = low_ref[:, ranks:].astype(jnp.float32)
    wide = 2 if lanes % 2 == 0 else 1
    size = wide * LANE

    @pl.loop(0, lanes // wide)
    def _(g):
        cols = pl.ds(pl.multiple_of(g * size, size), size)
        raw = jnp.dot(
            low_dt, proj_ref[:, cols], preferred_element_type=jnp.float32
        ) + bias_ref[:, cols]
        value = jnp.maximum(raw, 0.0) + jnp.log1p(jnp.exp(-jnp.abs(raw)))
        pushed = value * conv_ref[:, cols]
        for w in range(wide):
            k = g * wide + w
            step[k] = value[:, w * LANE : (w + 1) * LANE]
            drive[k] = pushed[:, w * LANE : (w + 1) * LANE]

    def run(with_out):
        @pl.loop(0, lanes // wide)
        def _(g):
            for b in range(batch):
                rates = [
                    [
                        rate_ref[pl.ds(n, 1), pl.ds(pl.multiple_of((g * wide + w) * LANE, LANE), LANE)]
                        for n in range(nstate)
                    ]
                    for w in range(wide)
                ]

                def one(t, carry):
                    at = pl.ds(b * length + t, CHUNKS, stride=span)
                    both = maps[at, :]
                    held, extra = carry
                    held, extra = list(held), list(extra)
                    now = [step[g * wide + w, at, :] for w in range(wide)]
                    push = [drive[g * wide + w, at, :] for w in range(wide)]
                    acc = [None] * wide
                    for n in range(nstate):
                        into = jnp.broadcast_to(both[:, n : n + 1], (CHUNKS, LANE))
                        if with_out:
                            outof = jnp.broadcast_to(
                                both[:, nstate + n : nstate + n + 1], (CHUNKS, LANE)
                            )
                        for w in range(wide):
                            i = w * nstate + n
                            held[i] = (
                                jnp.exp(-now[w] * rates[w][n]) * held[i] + push[w] * into
                            )
                            if with_out:
                                term = held[i] * outof
                                acc[w] = term if acc[w] is None else acc[w] + term
                    for w in range(wide):
                        if with_out:
                            result[g * wide + w, at, :] = acc[w]
                        else:
                            extra[w] = extra[w] + now[w]
                    return tuple(held), tuple(extra)

                zero = jnp.zeros((CHUNKS, LANE), jnp.float32)
                if with_out:
                    first = tuple(
                        state[b, g * wide + w, pl.ds(n * CHUNKS, CHUNKS), :]
                        for w in range(wide) for n in range(nstate)
                    )
                    lax.fori_loop(0, span, one, (first, ()))
                else:
                    held, extra = lax.fori_loop(
                        0, span, one, ((zero,) * (wide * nstate), (zero,) * wide)
                    )
                    for w in range(wide):
                        for n in range(nstate):
                            state[b, g * wide + w, pl.ds(n * CHUNKS, CHUNKS), :] = held[
                                w * nstate + n
                            ]
                        sums[b, g * wide + w] = extra[w]

    run(False)

    @pl.loop(0, lanes)
    def _(k):
        cols = pl.ds(pl.multiple_of(k * LANE, LANE), LANE)
        rate = rate_ref[:, cols]
        for b in range(batch):
            carry = jnp.zeros((nstate, LANE), jnp.float32)
            for c in range(CHUNKS):
                part = state[b, k, pl.ds(c, nstate, stride=CHUNKS), :]
                carry = jnp.exp(-sums[b, k, pl.ds(c, 1), :] * rate) * carry + part
            agg[pl.ds(b * nstate, nstate), cols] = carry.astype(jnp.bfloat16)
            tot[pl.ds(b, 1), cols] = jnp.sum(sums[b, k], axis=0, keepdims=True)

    def pair(source, target):
        device = {"dp": target}
        return (
            remote(agg, agg_in.at[source], s1.at[target], r1.at[source], device),
            remote(tot, tot_in.at[source], s2.at[target], r2.at[source], device),
        )

    for other in range(nd):
        @pl.when(other > me)
        def _():
            for copy in pair(me, other):
                copy.start()

    for other in range(nd):
        @pl.when(other < me)
        def _():
            for copy in pair(other, me):
                copy.wait_recv()

    @pl.loop(0, lanes)
    def _(k):
        cols = pl.ds(pl.multiple_of(k * LANE, LANE), LANE)
        rate = rate_ref[:, cols]
        for b in range(batch):
            def earlier(d, carry):
                decay = jnp.exp(-tot_in[d, pl.ds(b, 1), cols] * rate)
                return decay * carry + agg_in[d, pl.ds(b * nstate, nstate), cols].astype(
                    jnp.float32
                )

            carry = lax.fori_loop(0, me, earlier, jnp.zeros((nstate, LANE), jnp.float32))
            for c in range(CHUNKS):
                at = pl.ds(c, nstate, stride=CHUNKS)
                part = state[b, k, at, :]
                state[b, k, at, :] = carry
                carry = jnp.exp(-sums[b, k, pl.ds(c, 1), :] * rate) * carry + part

    run(True)

    @pl.loop(0, lanes)
    def _(k):
        out_ref[:, pl.ds(pl.multiple_of(k * LANE, LANE), LANE)] = result[k]

    for other in range(nd):
        @pl.when(other > me)
        def _():
            for copy in pair(me, other):
                copy.wait_send()


def scan(low, proj, bias, conv, rate, batch, nd, ranks):
    rows, chans = conv.shape
    nstate = rate.shape[0]
    lanes = chans // LANE
    big = pltpu.VMEM((lanes, rows, LANE), jnp.float32)
    return call(
        functools.partial(scan_kernel, nd, batch, nstate, ranks),
        jax.ShapeDtypeStruct((rows, chans), jnp.float32),
        [
            big, big,
            pltpu.VMEM((rows, low.shape[1] - ranks), jnp.float32),
            big,
            pltpu.VMEM((batch, lanes, nstate * CHUNKS, LANE), jnp.float32),
            pltpu.VMEM((batch, lanes, CHUNKS, LANE), jnp.float32),
            pltpu.VMEM((batch * nstate, chans), jnp.bfloat16),
            pltpu.VMEM((batch, chans), jnp.float32),
            pltpu.VMEM((nd, batch * nstate, chans), jnp.bfloat16),
            pltpu.VMEM((nd, batch, chans), jnp.float32),
        ] + [pltpu.SemaphoreType.DMA((nd,))] * 4,
        2, 30, "scan",
    )(low, proj, bias, conv, rate)


def out_kernel(nv, gated_ref, w_ref, resid_ref, out_ref, sent, recv, mine, s1, r1, s2, r2):
    me = lax.axis_index("vocab")
    rows, width = resid_ref.shape
    share = width // nv
    greet(("vocab",))

    def columns(index):
        return pl.ds(pl.multiple_of(index * share, share), share)

    tile = min(512, share)

    def product(index, put):
        @pl.loop(0, share // tile)
        def _(k):
            at = pl.multiple_of(index * share + k * tile, tile)
            put(
                pl.ds(pl.multiple_of(k * tile, tile), tile), pl.ds(at, tile),
                jnp.dot(
                    gated_ref[...], w_ref[:, pl.ds(at, tile)], preferred_element_type=jnp.float32
                ),
            )

    copies = {}
    order = sorted(range(1, nv), key=lambda s: abs(s - nv / 2))
    for shift in order:
        def put(local, whole, value):
            sent[shift - 1, :, local] = value.astype(jnp.bfloat16)

        product(lax.rem(me + shift, nv), put)
        copy = remote(
            sent.at[shift - 1], recv.at[shift - 1],
            s1.at[shift - 1], r1.at[shift - 1], peer("vocab", shift),
        )
        copy.start()
        copies[shift] = copy

    def put(local, whole, value):
        mine[:, local] = value

    product(me, put)
    for shift in order:
        copies[shift].wait()

    @pl.loop(0, share // tile)
    def _(k):
        local = pl.ds(pl.multiple_of(k * tile, tile), tile)
        whole = pl.ds(pl.multiple_of(me * share + k * tile, tile), tile)
        total = mine[:, local]
        for shift in range(1, nv):
            total = total + recv[shift - 1, :, local].astype(jnp.float32)
        hidden = (resid_ref[:, whole].astype(jnp.float32) + total).astype(jnp.bfloat16)
        sent[nv - 1, :, local] = hidden
        out_ref[:, whole] = hidden

    copies = []
    for shift in range(1, nv):
        copy = remote(
            sent.at[nv - 1], out_ref.at[:, columns(me)],
            s2.at[shift - 1], r2.at[shift - 1], peer("vocab", shift),
        )
        copy.start()
        copies.append(copy)
    for copy in copies:
        copy.wait()


def out_reduce(gated, w, resid, nv):
    rows, width = resid.shape
    share = width // nv
    sems = [pltpu.SemaphoreType.DMA((nv - 1,))] * 4
    return call(
        functools.partial(out_kernel, nv),
        jax.ShapeDtypeStruct((rows, width), jnp.bfloat16),
        [
            pltpu.VMEM((nv, rows, share), jnp.bfloat16),
            pltpu.VMEM((nv - 1, rows, share), jnp.bfloat16),
            pltpu.VMEM((rows, share), jnp.float32),
        ] + sems,
        3, 60, "out_reduce",
    )(gated, w, resid)


def tail_kernel(nv, nd, stats_ref, mask_ref, logp_ref, sum_ref, recv, part, parts, s1, r1, s2, r2):
    greet(("vocab", "dp"))
    copies = []
    for shift in range(1, nv):
        copy = remote(
            stats_ref, recv.at[shift - 1], s1.at[shift - 1], r1.at[shift - 1],
            peer("vocab", shift),
        )
        copy.start()
        copies.append(copy)
    for copy in copies:
        copy.wait()
    everyone = [stats_ref[...]] + [recv[k] for k in range(nv - 1)]
    top = everyone[0][0:1]
    for stats in everyone[1:]:
        top = jnp.maximum(top, stats[0:1])
    total = jnp.zeros_like(top)
    picked = jnp.zeros_like(top)
    for stats in everyone:
        total = total + stats[1:2] * jnp.exp(stats[0:1] - top)
        picked = picked + stats[2:3]
    logp = picked - (top + jnp.log(total))
    logp_ref[...] = logp
    masked = jnp.sum(jnp.where(mask_ref[...] > 0.0, logp, 0.0), axis=-1, keepdims=True)
    part[...] = jnp.broadcast_to(masked, part.shape)
    copies = []
    for shift in range(1, nd):
        copy = remote(
            part, parts.at[shift - 1], s2.at[shift - 1], r2.at[shift - 1], peer("dp", shift)
        )
        copy.start()
        copies.append(copy)
    grand = part[...]
    for shift in range(1, nd):
        copies[shift - 1].wait()
        grand = grand + parts[shift - 1]
    sum_ref[...] = grand


def tail(stats, mask, nv, nd):
    rows = stats.shape[1]
    return call(
        functools.partial(tail_kernel, nv, nd),
        (
            jax.ShapeDtypeStruct((1, rows), jnp.float32),
            jax.ShapeDtypeStruct((8, 128), jnp.float32),
        ),
        [
            pltpu.VMEM((nv - 1, 8, rows), jnp.float32),
            pltpu.VMEM((8, 128), jnp.float32),
            pltpu.VMEM((nd - 1, 8, 128), jnp.float32),
        ] + [pltpu.SemaphoreType.DMA((nv - 1,))] * 2 + [pltpu.SemaphoreType.DMA((nd - 1,))] * 2,
        4, 6, "tail",
    )(stats, mask)


def rms_norm(values, gain, epsilon):
    return values * lax.rsqrt(jnp.mean(values * values, axis=-1, keepdims=True) + epsilon) * gain


def body(
    resid, norm_gain, in_x, in_z, conv_w, conv_b, xdt_w, xbc_w, dt_gain, dt_proj, dt_bias,
    a_rate, out_w, final_gain, head_w, targets, lengths,
):
    nv, nd = lax.axis_size("vocab"), lax.axis_size("dp")
    batch, local_len, width = resid.shape
    channels = in_x.shape[1]
    nstate = a_rate.shape[1]
    ranks = xdt_w.shape[1]
    kernel_len = conv_w.shape[0]
    rows = batch * local_len
    vocab_index = lax.axis_index("vocab")

    full_x = lax.all_gather(in_x, "dp", axis=0, tiled=True)
    in_z, _ = lax.optimization_barrier((in_z, in_x))
    full_z = lax.all_gather(in_z, "dp", axis=0, tiled=True)
    full_head = lax.all_gather(head_w, "dp", axis=1, tiled=True)

    pad = -(2 * nstate) % 128
    low_w = jnp.concatenate([xdt_w, xbc_w, jnp.zeros((channels, pad), jnp.bfloat16)], axis=1)
    flat = resid.reshape(rows, width)
    stream = flat.astype(jnp.float32)
    normed = rms_norm(stream, norm_gain, 1e-05).astype(jnp.bfloat16)
    x_inner = (
        jnp.dot(normed, full_x, preferred_element_type=jnp.float32)
        .astype(jnp.bfloat16)
        .reshape(batch, local_len, channels)
    )
    before = lax.ppermute(
        x_inner[:, local_len - (kernel_len - 1) :, :], "dp", [(i, i + 1) for i in range(nd - 1)]
    )
    padded = jnp.concatenate([before, x_inner], axis=1).astype(jnp.float32)
    conv_sum = jnp.zeros((batch, local_len, channels), jnp.float32) + conv_b
    for tap in range(kernel_len):
        conv_sum = conv_sum + conv_w[tap] * padded[:, tap : tap + local_len, :]
    conv_act = jax.nn.silu(conv_sum).reshape(rows, channels)
    part = jnp.dot(
        conv_act.astype(jnp.bfloat16), low_w, preferred_element_type=jnp.float32
    ).astype(jnp.bfloat16)
    low = dt_reduce(part, dt_gain[None, :], nv, ranks)
    mixed = scan(low, dt_proj, dt_bias[None, :], conv_act, a_rate.T, batch, nd, ranks)
    z_gate = (
        jnp.dot(normed, full_z, preferred_element_type=jnp.float32)
        .astype(jnp.bfloat16)
        .astype(jnp.float32)
    )
    gated = (mixed * jax.nn.silu(z_gate)).astype(jnp.bfloat16)
    hidden = out_reduce(gated, out_w, flat, nv)
    share = width // nv
    hidden_share = lax.dynamic_slice_in_dim(hidden, vocab_index * share, share, 1)
    final = rms_norm(hidden.astype(jnp.float32), final_gain, 1e-05).astype(jnp.bfloat16)
    logits = lax.dot_general(
        final, full_head, (((1,), (1,)), ((), ())), preferred_element_type=jnp.float32
    )
    vocab_rows = head_w.shape[0]
    local_ids = targets.reshape(rows) - vocab_index * vocab_rows
    entry_ids = lax.broadcasted_iota(jnp.int32, (rows, vocab_rows), 1)
    picked = jnp.sum(jnp.where(entry_ids == local_ids[:, None], logits, 0.0), axis=-1)
    top = jnp.max(logits, axis=-1)
    total = jnp.sum(jnp.exp(logits - top[:, None]), axis=-1)
    stats = jnp.concatenate(
        [top[None], total[None], picked[None], jnp.zeros((5, rows), jnp.float32)], axis=0
    )
    positions = lax.axis_index("dp") * local_len + jnp.arange(local_len, dtype=jnp.int32)
    mask = (positions[None, :] < lengths[:, None]).astype(jnp.float32).reshape(1, rows)
    logp, grand = tail(stats, mask, nv, nd)
    mean_logp = grand[0, 0] / jnp.sum(lengths.astype(jnp.float32))
    return (
        hidden_share.reshape(batch, local_len, share),
        logp.reshape(batch, local_len),
        mean_logp,
    )


def solution(mesh):
    in_specs = (
        P(None, "dp", None), P(), P("dp", "vocab"), P("dp", "vocab"), P(None, "vocab"), P("vocab"),
        P("vocab", None), P("vocab", None), P(), P(None, "vocab"), P("vocab"), P("vocab", None),
        P("vocab", None), P(), P("vocab", "dp"), P(None, "dp"), P(),
    )
    out_specs = (P(None, "dp", "vocab"), P(None, "dp"), P())
    return jax.shard_map(body, mesh=mesh, in_specs=in_specs, out_specs=out_specs, check_vma=False)
```

```python
import functools

import jax
import jax.numpy as jnp
from jax import lax
from jax.experimental import pallas as pl
from jax.experimental.pallas import tpu as pltpu
from jax.sharding import PartitionSpec as P

MESH = pl.DeviceIdType.MESH
VMEM = pl.BlockSpec(memory_space=pltpu.VMEM)
CHUNKS = 8
LANE = 128
PIECES = 8
LAG = 8
LOG2E = 1.4426950408889634


def peer(axis, shift):
    size = lax.axis_size(axis)
    return {axis: lax.rem(lax.axis_index(axis) + shift, size)}


def greet(axes):
    barrier = pltpu.get_barrier_semaphore()
    count = 0
    for axis in axes:
        for shift in range(1, lax.axis_size(axis)):
            pl.semaphore_signal(barrier, inc=1, device_id=peer(axis, shift), device_id_type=MESH)
            count += 1
    pl.semaphore_wait(barrier, count)


def remote(src, dst, send_sem, recv_sem, device):
    return pltpu.make_async_remote_copy(
        src_ref=src, dst_ref=dst, send_sem=send_sem, recv_sem=recv_sem,
        device_id=device, device_id_type=MESH,
    )


def call(kernel, out_shape, scratch, cid, cost_us, name):
    return pl.pallas_call(
        kernel,
        out_shape=out_shape,
        scratch_shapes=scratch,
        compiler_params=pltpu.CompilerParams(
            collective_id=cid, has_side_effects=True, vmem_limit_bytes=56 * 1024 * 1024
        ),
        cost_estimate=pl.CostEstimate(
            flops=0, bytes_accessed=int(cost_us * 3.0e6), transcendentals=0
        ),
        name=name,
    )


def dt_kernel(nv, ranks, part_ref, gain_ref, out_ref, recv, mine, s1, r1, s2, r2):
    me = lax.axis_index("vocab")
    rows = part_ref.shape[0] // nv
    greet(("vocab",))
    copies = []
    for shift in range(1, nv):
        target = lax.rem(me + shift, nv)
        copy = remote(
            part_ref.at[pl.ds(pl.multiple_of(target * rows, rows), rows)], recv.at[shift - 1],
            s1.at[shift - 1], r1.at[shift - 1], peer("vocab", shift),
        )
        copy.start()
        copies.append(copy)
    own = pl.ds(pl.multiple_of(me * rows, rows), rows)
    total = part_ref[own, :].astype(jnp.float32)
    for shift in range(1, nv):
        copies[shift - 1].wait()
        total = total + recv[shift - 1].astype(jnp.float32)
    dt = total[:, :ranks]
    scale = lax.rsqrt(jnp.mean(dt * dt, axis=-1, keepdims=True) + 1e-06)
    mine[:, :ranks] = (dt * scale * gain_ref[...]).astype(jnp.bfloat16)
    mine[:, ranks:] = total[:, ranks:].astype(jnp.bfloat16)
    copies = []
    for shift in range(1, nv):
        copy = remote(
            mine, out_ref.at[own], s2.at[shift - 1], r2.at[shift - 1], peer("vocab", shift)
        )
        copy.start()
        copies.append(copy)
    out_ref[own, :] = mine[...]
    for copy in copies:
        copy.wait()


def dt_reduce(part, gain, nv, ranks):
    rows, cols = part.shape
    sems = [pltpu.SemaphoreType.DMA((nv - 1,))] * 4
    return call(
        functools.partial(dt_kernel, nv, ranks),
        jax.ShapeDtypeStruct((rows, cols), jnp.bfloat16),
        [
            pltpu.VMEM((nv - 1, rows // nv, cols), jnp.bfloat16),
            pltpu.VMEM((rows // nv, cols), jnp.bfloat16),
        ] + sems,
        1, 10, "dt_reduce",
    )(part, gain)


def scan_kernel(
    nd, batch, nstate, ranks, low_ref, proj_ref, bias_ref, conv_ref, rate_ref, out_ref,
    step, drive, maps, result, state, sums, agg, tot, agg_in, tot_in, s1, r1, s2, r2,
):
    me = lax.axis_index("dp")
    rows, chans = conv_ref.shape
    lanes = chans // LANE
    length = rows // batch
    span = length // CHUNKS
    greet(("dp",))
    low_dt = low_ref[:, :ranks]
    maps[...] = low_ref[:, ranks:].astype(jnp.float32)
    wide = 2 if lanes % 2 == 0 else 1
    size = wide * LANE

    @pl.loop(0, lanes // wide)
    def _(g):
        cols = pl.ds(pl.multiple_of(g * size, size), size)
        raw = jnp.dot(
            low_dt, proj_ref[:, cols], preferred_element_type=jnp.float32
        ) + bias_ref[:, cols]
        value = jnp.maximum(raw, 0.0) + jnp.log1p(jnp.exp(-jnp.abs(raw)))
        pushed = value * conv_ref[:, cols]
        for w in range(wide):
            k = g * wide + w
            step[k] = value[:, w * LANE : (w + 1) * LANE]
            drive[k] = pushed[:, w * LANE : (w + 1) * LANE]

    def run(with_out):
        @pl.loop(0, lanes // wide)
        def _(g):
            for b in range(batch):
                rates = [
                    [
                        rate_ref[pl.ds(n, 1), pl.ds(pl.multiple_of((g * wide + w) * LANE, LANE), LANE)]
                        * -LOG2E
                        for n in range(nstate)
                    ]
                    for w in range(wide)
                ]

                def one(t, carry):
                    at = pl.ds(b * length + t, CHUNKS, stride=span)
                    both = maps[at, :]
                    held, extra = carry
                    held, extra = list(held), list(extra)
                    now = [step[g * wide + w, at, :] for w in range(wide)]
                    push = [drive[g * wide + w, at, :] for w in range(wide)]
                    acc = [None] * wide
                    for n in range(nstate):
                        into = jnp.broadcast_to(both[:, n : n + 1], (CHUNKS, LANE))
                        if with_out:
                            outof = jnp.broadcast_to(
                                both[:, nstate + n : nstate + n + 1], (CHUNKS, LANE)
                            )
                        for w in range(wide):
                            i = w * nstate + n
                            held[i] = (
                                jnp.exp2(now[w] * rates[w][n]) * held[i] + push[w] * into
                            )
                            if with_out:
                                term = held[i] * outof
                                acc[w] = term if acc[w] is None else acc[w] + term
                    for w in range(wide):
                        if with_out:
                            result[g * wide + w, at, :] = acc[w]
                        else:
                            extra[w] = extra[w] + now[w]
                    return tuple(held), tuple(extra)

                zero = jnp.zeros((CHUNKS, LANE), jnp.float32)
                if with_out:
                    first = tuple(
                        state[b, g * wide + w, pl.ds(n * CHUNKS, CHUNKS), :]
                        for w in range(wide) for n in range(nstate)
                    )
                    lax.fori_loop(0, span, one, (first, ()))
                else:
                    held, extra = lax.fori_loop(
                        0, span, one, ((zero,) * (wide * nstate), (zero,) * wide)
                    )
                    for w in range(wide):
                        for n in range(nstate):
                            state[b, g * wide + w, pl.ds(n * CHUNKS, CHUNKS), :] = held[
                                w * nstate + n
                            ]
                        sums[b, g * wide + w] = extra[w]

    run(False)

    @pl.loop(0, lanes)
    def _(k):
        cols = pl.ds(pl.multiple_of(k * LANE, LANE), LANE)
        rate = rate_ref[:, cols]
        for b in range(batch):
            carry = jnp.zeros((nstate, LANE), jnp.float32)
            for c in range(CHUNKS):
                part = state[b, k, pl.ds(c, nstate, stride=CHUNKS), :]
                carry = jnp.exp(-sums[b, k, pl.ds(c, 1), :] * rate) * carry + part
            agg[pl.ds(b * nstate, nstate), cols] = carry.astype(jnp.bfloat16)
            tot[pl.ds(b, 1), cols] = jnp.sum(sums[b, k], axis=0, keepdims=True)

    def pair(source, target):
        device = {"dp": target}
        return (
            remote(agg, agg_in.at[source], s1.at[target], r1.at[source], device),
            remote(tot, tot_in.at[source], s2.at[target], r2.at[source], device),
        )

    for other in range(nd):
        @pl.when(other > me)
        def _():
            for copy in pair(me, other):
                copy.start()

    for other in range(nd):
        @pl.when(other < me)
        def _():
            for copy in pair(other, me):
                copy.wait_recv()

    group = 4 if lanes % 4 == 0 else 1

    @pl.loop(0, lanes // group)
    def _(g):
        cols = [pl.ds(pl.multiple_of((g * group + w) * LANE, LANE), LANE) for w in range(group)]
        rate = [rate_ref[:, at] for at in cols]
        every = [(b, w) for b in range(batch) for w in range(group)]

        def earlier(d, carry):
            return tuple(
                jnp.exp(-tot_in[d, pl.ds(b, 1), cols[w]] * rate[w]) * held
                + agg_in[d, pl.ds(b * nstate, nstate), cols[w]].astype(jnp.float32)
                for (b, w), held in zip(every, carry)
            )

        zero = jnp.zeros((nstate, LANE), jnp.float32)
        starts = lax.fori_loop(0, me, earlier, (zero,) * len(every))
        for (b, w), carry in zip(every, starts):
            k = g * group + w
            for c in range(CHUNKS):
                at = pl.ds(c, nstate, stride=CHUNKS)
                part = state[b, k, at, :]
                state[b, k, at, :] = carry
                carry = jnp.exp(-sums[b, k, pl.ds(c, 1), :] * rate[w]) * carry + part

    run(True)

    @pl.loop(0, lanes)
    def _(k):
        out_ref[:, pl.ds(pl.multiple_of(k * LANE, LANE), LANE)] = result[k]

    for other in range(nd):
        @pl.when(other > me)
        def _():
            for copy in pair(me, other):
                copy.wait_send()


def scan(low, proj, bias, conv, rate, batch, nd, ranks):
    rows, chans = conv.shape
    nstate = rate.shape[0]
    lanes = chans // LANE
    big = pltpu.VMEM((lanes, rows, LANE), jnp.float32)
    return call(
        functools.partial(scan_kernel, nd, batch, nstate, ranks),
        jax.ShapeDtypeStruct((rows, chans), jnp.float32),
        [
            big, big,
            pltpu.VMEM((rows, low.shape[1] - ranks), jnp.float32),
            big,
            pltpu.VMEM((batch, lanes, nstate * CHUNKS, LANE), jnp.float32),
            pltpu.VMEM((batch, lanes, CHUNKS, LANE), jnp.float32),
            pltpu.VMEM((batch * nstate, chans), jnp.bfloat16),
            pltpu.VMEM((batch, chans), jnp.float32),
            pltpu.VMEM((nd, batch * nstate, chans), jnp.bfloat16),
            pltpu.VMEM((nd, batch, chans), jnp.float32),
        ] + [pltpu.SemaphoreType.DMA((nd,))] * 4,
        2, 30, "scan",
    )(low, proj, bias, conv, rate)


def out_kernel(nv, gated_ref, w_ref, resid_ref, out_ref, mine, sent, recv, s1, r1, s2, r2):
    me = lax.axis_index("vocab")
    rows, width = resid_ref.shape
    half = width // 2
    block = rows // PIECES
    right = {"vocab": lax.rem(me + 1, nv)}
    left = {"vocab": lax.rem(me + nv - 1, nv)}
    barrier = pltpu.get_barrier_semaphore()

    for place, device in ((me < nv - 1, right), (me > 0, left)):
        @pl.when(place)
        def _():
            pl.semaphore_signal(barrier, inc=1, device_id=device, device_id_type=MESH)

    tile = min(512, half)

    @pl.loop(0, width // tile)
    def _(k):
        cols = pl.ds(pl.multiple_of(k * tile, tile), tile)
        mine[:, cols] = jnp.dot(
            gated_ref[...], w_ref[:, cols], preferred_element_type=jnp.float32
        )

    at_end = jnp.logical_or(me == 0, me == nv - 1)

    @pl.when(at_end)
    def _():
        pl.semaphore_wait(barrier, 1)

    @pl.when(jnp.logical_not(at_end))
    def _():
        pl.semaphore_wait(barrier, 2)

    ways = ((me, right, left), (nv - 1 - me, left, right))

    def up_copy(h, c):
        at = pl.ds(c * block, block)
        return remote(
            sent.at[h, at], recv.at[h, at], s1.at[h, c], r1.at[h, c], ways[h][1]
        )

    def down_copy(h, c):
        view = out_ref.at[pl.ds(c * block, block), pl.ds(h * half, half)]
        return remote(view, view, s2.at[h, c], r2.at[h, c], ways[h][2])

    def up(h, c):
        place = ways[h][0]
        at = pl.ds(c * block, block)
        cols = pl.ds(h * half, half)

        @pl.when(place > 0)
        def _():
            up_copy(h, c).wait_recv()
            mine[at, cols] = mine[at, cols] + recv[h, at, :].astype(jnp.float32)

        @pl.when(place < nv - 1)
        def _():
            sent[h, at, :] = mine[at, cols].astype(jnp.bfloat16)
            up_copy(h, c).start()

        @pl.when(place == nv - 1)
        def _():
            out_ref[at, cols] = (
                resid_ref[at, cols].astype(jnp.float32) + mine[at, cols]
            ).astype(jnp.bfloat16)
            down_copy(h, c).start()

    def down(h, c):
        place = ways[h][0]

        @pl.when(place < nv - 1)
        def _():
            down_copy(h, c).wait_recv()

            @pl.when(place > 0)
            def _():
                down_copy(h, c).start()

    for step in range(PIECES + LAG):
        if step < PIECES:
            up(0, step)
            up(1, step)
        if step >= LAG:
            down(0, step - LAG)
            down(1, step - LAG)
    for h in range(2):
        place = ways[h][0]
        for c in range(PIECES):
            @pl.when(place < nv - 1)
            def _():
                up_copy(h, c).wait_send()

            @pl.when(place > 0)
            def _():
                down_copy(h, c).wait_send()


def out_reduce(gated, w, resid, nv):
    rows, width = resid.shape
    sems = [pltpu.SemaphoreType.DMA((2, PIECES))] * 4
    return call(
        functools.partial(out_kernel, nv),
        jax.ShapeDtypeStruct((rows, width), jnp.bfloat16),
        [
            pltpu.VMEM((rows, width), jnp.float32),
            pltpu.VMEM((2, rows, width // 2), jnp.bfloat16),
            pltpu.VMEM((2, rows, width // 2), jnp.bfloat16),
        ] + sems,
        3, 60, "out_reduce",
    )(gated, w, resid)


def tail_kernel(nv, nd, stats_ref, mask_ref, logp_ref, sum_ref, recv, part, parts, s1, r1, s2, r2):
    greet(("vocab", "dp"))
    copies = []
    for shift in range(1, nv):
        copy = remote(
            stats_ref, recv.at[shift - 1], s1.at[shift - 1], r1.at[shift - 1],
            peer("vocab", shift),
        )
        copy.start()
        copies.append(copy)
    for copy in copies:
        copy.wait()
    everyone = [stats_ref[...]] + [recv[k] for k in range(nv - 1)]
    top = everyone[0][0:1]
    for stats in everyone[1:]:
        top = jnp.maximum(top, stats[0:1])
    total = jnp.zeros_like(top)
    picked = jnp.zeros_like(top)
    for stats in everyone:
        total = total + stats[1:2] * jnp.exp(stats[0:1] - top)
        picked = picked + stats[2:3]
    logp = picked - (top + jnp.log(total))
    logp_ref[...] = logp
    masked = jnp.sum(jnp.where(mask_ref[...] > 0.0, logp, 0.0), axis=-1, keepdims=True)
    part[...] = jnp.broadcast_to(masked, part.shape)
    copies = []
    for shift in range(1, nd):
        copy = remote(
            part, parts.at[shift - 1], s2.at[shift - 1], r2.at[shift - 1], peer("dp", shift)
        )
        copy.start()
        copies.append(copy)
    grand = part[...]
    for shift in range(1, nd):
        copies[shift - 1].wait()
        grand = grand + parts[shift - 1]
    sum_ref[...] = grand


def tail(stats, mask, nv, nd):
    rows = stats.shape[1]
    return call(
        functools.partial(tail_kernel, nv, nd),
        (
            jax.ShapeDtypeStruct((1, rows), jnp.float32),
            jax.ShapeDtypeStruct((8, 128), jnp.float32),
        ),
        [
            pltpu.VMEM((nv - 1, 8, rows), jnp.float32),
            pltpu.VMEM((8, 128), jnp.float32),
            pltpu.VMEM((nd - 1, 8, 128), jnp.float32),
        ] + [pltpu.SemaphoreType.DMA((nv - 1,))] * 2 + [pltpu.SemaphoreType.DMA((nd - 1,))] * 2,
        4, 6, "tail",
    )(stats, mask)


def rms_norm(values, gain, epsilon):
    return values * lax.rsqrt(jnp.mean(values * values, axis=-1, keepdims=True) + epsilon) * gain


def body(
    resid, norm_gain, in_x, in_z, conv_w, conv_b, xdt_w, xbc_w, dt_gain, dt_proj, dt_bias,
    a_rate, out_w, final_gain, head_w, targets, lengths,
):
    nv, nd = lax.axis_size("vocab"), lax.axis_size("dp")
    batch, local_len, width = resid.shape
    channels = in_x.shape[1]
    nstate = a_rate.shape[1]
    ranks = xdt_w.shape[1]
    kernel_len = conv_w.shape[0]
    rows = batch * local_len
    vocab_index = lax.axis_index("vocab")

    full_x = lax.all_gather(in_x, "dp", axis=0, tiled=True)
    in_z, _ = lax.optimization_barrier((in_z, in_x))
    full_z = lax.all_gather(in_z, "dp", axis=0, tiled=True)
    full_head = lax.all_gather(head_w, "dp", axis=1, tiled=True)

    pad = -(2 * nstate) % 128
    low_w = jnp.concatenate([xdt_w, xbc_w, jnp.zeros((channels, pad), jnp.bfloat16)], axis=1)
    flat = resid.reshape(rows, width)
    stream = flat.astype(jnp.float32)
    normed = rms_norm(stream, norm_gain, 1e-05).astype(jnp.bfloat16)
    x_inner = (
        jnp.dot(normed, full_x, preferred_element_type=jnp.float32)
        .astype(jnp.bfloat16)
        .reshape(batch, local_len, channels)
    )
    before = lax.ppermute(
        x_inner[:, local_len - (kernel_len - 1) :, :], "dp", [(i, i + 1) for i in range(nd - 1)]
    )
    padded = jnp.concatenate([before, x_inner], axis=1).astype(jnp.float32)
    conv_sum = jnp.zeros((batch, local_len, channels), jnp.float32) + conv_b
    for tap in range(kernel_len):
        conv_sum = conv_sum + conv_w[tap] * padded[:, tap : tap + local_len, :]
    conv_act = jax.nn.silu(conv_sum).reshape(rows, channels)
    part = jnp.dot(
        conv_act.astype(jnp.bfloat16), low_w, preferred_element_type=jnp.float32
    ).astype(jnp.bfloat16)
    low = dt_reduce(part, dt_gain[None, :], nv, ranks)
    mixed = scan(low, dt_proj, dt_bias[None, :], conv_act, a_rate.T, batch, nd, ranks)
    z_gate = (
        jnp.dot(normed, full_z, preferred_element_type=jnp.float32)
        .astype(jnp.bfloat16)
        .astype(jnp.float32)
    )
    gated = (mixed * jax.nn.silu(z_gate)).astype(jnp.bfloat16)
    hidden = out_reduce(gated, out_w, flat, nv)
    share = width // nv
    hidden_share = lax.dynamic_slice_in_dim(hidden, vocab_index * share, share, 1)
    final = rms_norm(hidden.astype(jnp.float32), final_gain, 1e-05).astype(jnp.bfloat16)
    logits = lax.dot_general(
        final, full_head, (((1,), (1,)), ((), ())), preferred_element_type=jnp.float32
    )
    vocab_rows = head_w.shape[0]
    local_ids = targets.reshape(rows) - vocab_index * vocab_rows
    entry_ids = lax.broadcasted_iota(jnp.int32, (rows, vocab_rows), 1)
    picked = jnp.sum(jnp.where(entry_ids == local_ids[:, None], logits, 0.0), axis=-1)
    top = jnp.max(logits, axis=-1)
    total = jnp.sum(jnp.exp(logits - top[:, None]), axis=-1)
    stats = jnp.concatenate(
        [top[None], total[None], picked[None], jnp.zeros((5, rows), jnp.float32)], axis=0
    )
    positions = lax.axis_index("dp") * local_len + jnp.arange(local_len, dtype=jnp.int32)
    mask = (positions[None, :] < lengths[:, None]).astype(jnp.float32).reshape(1, rows)
    logp, grand = tail(stats, mask, nv, nd)
    mean_logp = grand[0, 0] / jnp.sum(lengths.astype(jnp.float32))
    return (
        hidden_share.reshape(batch, local_len, share),
        logp.reshape(batch, local_len),
        mean_logp,
    )


def solution(mesh):
    in_specs = (
        P(None, "dp", None), P(), P("dp", "vocab"), P("dp", "vocab"), P(None, "vocab"), P("vocab"),
        P("vocab", None), P("vocab", None), P(), P(None, "vocab"), P("vocab"), P("vocab", None),
        P("vocab", None), P(), P("vocab", "dp"), P(None, "dp"), P(),
    )
    out_specs = (P(None, "dp", "vocab"), P(None, "dp"), P())
    return jax.shard_map(body, mesh=mesh, in_specs=in_specs, out_specs=out_specs, check_vma=False)
```
